32 devices in a mesh: seq: 8 (over z, y), tensor: 4 (over x, core).
Axes of the slice: x: 2, y: 2, z: 4, core: 2. Of those that a mesh axis runs over, the one named last changes fastest.
Arguments:
- queries: bfloat16 [2048, 8192], P('seq', 'tensor'), may hold values from -4 to 4, as said below
- keys: bfloat16 [2048, 1024], P('seq', 'tensor'), may hold values from -96 to 96, as said below
- values: bfloat16 [2048, 1024], P('seq', 'tensor'), may hold values from -6 to 6
- block_pos: int32 [16], replicated, may hold values from 0 to 15, each once
Outputs:
- attended: bfloat16 [2048, 8192], P('seq')
The draws below stay inside these ranges and needn't reach their ends.
Inputs may be any that keep to these rules, and one draw needn't show every extreme that they name: block_pos is a permutation of 0 to 15. real-valued queries. real-valued keys.
All inputs are finite; a program needn't handle non-finite values.
Results may differ from the reference program's by a relative error of at most 0.004.
Values may be sent and summed in bfloat16 or wider, within the bound.
No kernel may reach another device: no remote copies, remote signals or barrier semaphores. Data moves between devices by JAX's collectives and lax.ppermute only.
A program may use at most 64 MiB of HBM per device.

```python
import math
import jax
import jax.numpy as jnp
from jax import lax

QUERY_HEADS = 64
KEY_VALUE_HEADS = 8
HEAD_WIDTH = 128
VISIBLE_SHARDS = 4
SHARD_TOKENS = 256
BLK = 128
NB = 16
SEQUENCE_TOKENS = 2048
N_SEQ = 8


def shared_fields(key):
    base = jax.random.fold_in(key, 7)
    key_q, key_sample = jax.random.split(base, 2)
    query_field = jnp.clip(jax.random.normal(key_q, (SEQUENCE_TOKENS, QUERY_HEADS * HEAD_WIDTH), jnp.float32), -4.0, 4.0)
    key_tensor = jnp.clip(jax.random.normal(key_sample, (SEQUENCE_TOKENS, KEY_VALUE_HEADS * HEAD_WIDTH), jnp.float32), -4.0, 4.0)
    return (query_field, key_tensor)


def draw_queries(key, part):
    return shared_fields(key)[0].astype(jnp.bfloat16)


def draw_keys(key, part):
    return shared_fields(key)[1].astype(jnp.bfloat16)


def block_scale(stream_key, extent, pieces, smallest, top_value):
    loudness, own = 1.0, jax.random.fold_in(stream_key, 6)
    for dim, parts in pieces:
        steps = jnp.exp(jax.random.uniform(jax.random.fold_in(own, dim), (parts,), jnp.float32, smallest / len(pieces), top_value / len(pieces)))
        loudness = loudness * jnp.repeat(steps, extent[dim] // parts).reshape([-1 if axis == dim else 1 for axis in range(len(extent))])
    return loudness


def scatter_about(own_key, extent, width, bound, cuts=(), kind=jnp.bfloat16):
    array = jax.random.normal(own_key, extent, jnp.float32) * width
    if len(cuts) > 0:
        array = block_scale(own_key, extent, cuts, -0.22, 0.18) * array
    return jnp.clip(array, min=-bound, max=bound).astype(kind)


def setup_inputs(seed: int = 0) -> dict:
    seeds = jax.random.split(jax.random.key(seed), 5)
    queries = draw_queries(jax.random.fold_in(seeds[4], 71), 0)
    keys = draw_keys(jax.random.fold_in(seeds[4], 71), 0)
    values = scatter_about(seeds[2], (SEQUENCE_TOKENS, KEY_VALUE_HEADS * HEAD_WIDTH), 1.0, 6.0, ((0, 8), (1, 4)))
    block_pos = jax.random.permutation(seeds[3], NB).astype(jnp.int32)
    return dict(queries=queries, keys=keys, values=values, block_pos=block_pos)


def reference(queries, keys, values, block_pos):
    group_factor = QUERY_HEADS // KEY_VALUE_HEADS
    scale = 1.0 / math.sqrt(HEAD_WIDTH)
    offsets = jnp.arange(BLK, dtype=jnp.int32)
    positions = (block_pos[:, None].astype(jnp.int32) * BLK + offsets[None, :]).reshape(-1)

    def one_shard(shard):
        start = (shard * SHARD_TOKENS).astype(jnp.int32)
        query_rows = lax.dynamic_slice_in_dim(queries, start, SHARD_TOKENS, 0).astype(jnp.float32)
        query_rows = query_rows.reshape(SHARD_TOKENS, KEY_VALUE_HEADS, group_factor, HEAD_WIDTH)
        q_pos = lax.dynamic_slice_in_dim(positions, start, SHARD_TOKENS, 0)
        key_collection = []
        value_collection = []
        pos_list = []
        for back in range(VISIBLE_SHARDS):
            source = ((shard - back) % N_SEQ * SHARD_TOKENS).astype(jnp.int32)
            key_collection.append(lax.dynamic_slice_in_dim(keys, source, SHARD_TOKENS, 0))
            value_collection.append(lax.dynamic_slice_in_dim(values, source, SHARD_TOKENS, 0))
            pos_list.append(lax.dynamic_slice_in_dim(positions, source, SHARD_TOKENS, 0))
        key_gathered = jnp.concatenate(key_collection, 0).astype(jnp.float32).reshape(VISIBLE_SHARDS * SHARD_TOKENS, KEY_VALUE_HEADS, HEAD_WIDTH)
        value_gathered = jnp.concatenate(value_collection, 0).astype(jnp.float32).reshape(VISIBLE_SHARDS * SHARD_TOKENS, KEY_VALUE_HEADS, HEAD_WIDTH)
        key_pos = jnp.concatenate(pos_list, 0)
        scores = jnp.einsum('qgrd,kgd->grqk', query_rows, key_gathered) * scale
        allowed = key_pos[None, :] <= q_pos[:, None]
        scores = jnp.where(allowed[None, None], scores, -1e+30)
        top = lax.optimization_barrier(jnp.max(scores, axis=-1, keepdims=True))
        weights = jnp.exp(scores - top)
        total = lax.optimization_barrier(jnp.sum(weights, axis=-1))
        rounded = lax.optimization_barrier(weights.astype(jnp.bfloat16)).astype(jnp.float32)
        mixed = jnp.einsum('grqk,kgd->qgrd', rounded, value_gathered)
        mixed = mixed / jnp.transpose(total, (2, 0, 1))[..., None]
        return mixed.reshape(SHARD_TOKENS, QUERY_HEADS * HEAD_WIDTH).astype(jnp.bfloat16)
    shards = lax.map(one_shard, jnp.arange(N_SEQ, dtype=jnp.int32))
    return shards.reshape(SEQUENCE_TOKENS, QUERY_HEADS * HEAD_WIDTH)
```

```python
import functools
import math

import jax
import jax.numpy as jnp
from jax import lax
from jax.experimental import pallas as pl
from jax.experimental.pallas import tpu as pltpu
from jax.sharding import PartitionSpec as P

QUERY_HEADS = 64
KEY_VALUE_HEADS = 8
HEAD_WIDTH = 128
GROUP = QUERY_HEADS // KEY_VALUE_HEADS
VISIBLE_SHARDS = 4


def shift(x, axis, distance):
    n = lax.axis_size(axis)
    return lax.ppermute(x, axis, [(i, (i + distance) % n) for i in range(n)])


def partner(x, axis):
    n = lax.axis_size(axis)
    return lax.ppermute(x, axis, [(i, i ^ 1) for i in range(n)])


def attend_kernel(shard_ref, pos_ref, q_ref, own_ref, two_ref, swap_ref, pair_ref, far_ref,
                  *rest, group, block_len, count):
    outs = rest[:2]
    k_scr, v_scr, bias_scr, q_scr, q_sem = rest[2:]
    tok = 2 * block_len
    width = GROUP * HEAD_WIDTH
    fetch = pltpu.make_async_copy(q_ref.at[:, group * width:(group + 1) * width], q_scr, q_sem)
    fetch.start()
    shard = shard_ref[0]
    odd = lax.rem(shard, 2)
    for slot, ref in enumerate((own_ref, two_ref, swap_ref)):
        k_scr[slot * tok:(slot + 1) * tok, :] = ref[0]
        v_scr[slot * tok:(slot + 1) * tok, :HEAD_WIDTH] = ref[1]

    @pl.when(odd == 1)
    def _():
        k_scr[3 * tok:, :] = pair_ref[0]
        v_scr[3 * tok:, :HEAD_WIDTH] = pair_ref[1]

    @pl.when(odd == 0)
    def _():
        k_scr[3 * tok:, :] = far_ref[0]
        v_scr[3 * tok:, :HEAD_WIDTH] = far_ref[1]

    v_scr[:, HEAD_WIDTH:] = jnp.ones((VISIBLE_SHARDS * tok, HEAD_WIDTH), jnp.bfloat16)
    backs = (0, 2, jnp.where(odd == 1, 3, 1), jnp.where(odd == 1, 1, 3))
    rows = lax.broadcasted_iota(jnp.int32, (block_len, block_len), 0)
    cols = lax.broadcasted_iota(jnp.int32, (block_len, block_len), 1)
    ahead = cols - rows
    for qb in range(2):
        q_block = pos_ref[2 * shard + qb]
        for slot in range(VISIBLE_SHARDS):
            source = lax.rem(shard - backs[slot] + count, count)
            for kb in range(2):
                gap = (pos_ref[2 * source + kb] - q_block) * block_len
                bias_scr[qb * block_len:(qb + 1) * block_len,
                         (2 * slot + kb) * block_len:(2 * slot + kb + 1) * block_len] = (
                    jnp.where(ahead + gap <= 0, 0.0, -1e30))

    fetch.wait()
    scale = 1.0 / math.sqrt(HEAD_WIDTH)
    for qb in range(2):
        def head(h, _):
            at = pl.ds(pl.multiple_of(h * HEAD_WIDTH, HEAD_WIDTH), HEAD_WIDTH)
            q = q_scr[qb * block_len:(qb + 1) * block_len, at]
            s = lax.dot_general(q, k_scr[...], (((1,), (1,)), ((), ())),
                                preferred_element_type=jnp.float32)
            s = s + bias_scr[qb * block_len:(qb + 1) * block_len, :]
            top = jnp.max(s, axis=1, keepdims=True)
            w = jnp.exp((s - top) * scale).astype(jnp.bfloat16)
            o = jnp.dot(w, v_scr[...], preferred_element_type=jnp.float32)
            outs[qb][:, at] = (o[:, :HEAD_WIDTH] / o[:, HEAD_WIDTH:]).astype(jnp.bfloat16)
            return 0
        lax.fori_loop(0, GROUP, head, 0, unroll=2)


def attend(shard, block_pos, queries, group, pieces):
    tok = queries.shape[0]
    block_len = tok // 2
    width = GROUP * HEAD_WIDTH
    vmem = pl.BlockSpec(memory_space=pltpu.VMEM)
    smem = pl.BlockSpec(memory_space=pltpu.SMEM)
    out = jax.ShapeDtypeStruct((block_len, width), jnp.bfloat16)
    return pl.pallas_call(
        functools.partial(attend_kernel, group=group, block_len=block_len,
                          count=lax.axis_size("seq")),
        in_specs=[smem, smem, pl.BlockSpec(memory_space=pl.ANY)] + [vmem] * 5,
        out_specs=[vmem, vmem],
        out_shape=[out, out],
        scratch_shapes=[
            pltpu.VMEM((VISIBLE_SHARDS * tok, HEAD_WIDTH), jnp.bfloat16),
            pltpu.VMEM((VISIBLE_SHARDS * tok, 2 * HEAD_WIDTH), jnp.bfloat16),
            pltpu.VMEM((tok, VISIBLE_SHARDS * tok), jnp.float32),
            pltpu.VMEM((tok, width), jnp.bfloat16),
            pltpu.SemaphoreType.DMA,
        ],
        name=f"attend{group}",
    )(shard, block_pos, queries, *pieces)


def place_kernel(col_ref, *refs, rows, n, aliased):
    chunks = refs[:n]
    out = refs[n + aliased]
    sems = refs[n + aliased + 1]
    copies = []
    for i, (chunk, row) in enumerate(zip(chunks, rows)):
        h, w = chunk.shape
        col = pl.multiple_of(col_ref[i] * w, w)
        copies.append(pltpu.make_async_copy(
            chunk, out.at[pl.ds(row, h), pl.ds(col, w)], sems.at[i]))
    for copy in copies:
        copy.start()
    for copy in copies:
        copy.wait()


def place(out, shape, entries):
    chunks = [e[0] for e in entries]
    rows = tuple(e[1] for e in entries)
    cols = jnp.stack([e[2] for e in entries]).astype(jnp.int32)
    n = len(chunks)
    aliased = 0 if out is None else 1
    any_spec = pl.BlockSpec(memory_space=pl.ANY)
    args = [cols] + chunks + ([] if out is None else [out])
    return pl.pallas_call(
        functools.partial(place_kernel, rows=rows, n=n, aliased=aliased),
        in_specs=[pl.BlockSpec(memory_space=pltpu.SMEM)]
        + [pl.BlockSpec(memory_space=pltpu.VMEM)] * n + [any_spec] * aliased,
        out_specs=any_spec,
        out_shape=jax.ShapeDtypeStruct(shape, jnp.bfloat16),
        input_output_aliases={n + 1: 0} if aliased else {},
        scratch_shapes=[pltpu.SemaphoreType.DMA((n,))],
        name="place",
    )(*args)


def body(queries, keys, values, block_pos):
    tok = queries.shape[0]
    block_len = tok // 2
    groups = keys.shape[1] // HEAD_WIDTH
    count = lax.axis_size("seq")
    tensor = lax.axis_size("tensor")
    shard = lax.axis_index("seq").astype(jnp.int32)
    me = lax.axis_index("tensor").astype(jnp.int32)
    shape = (tok, queries.shape[1] * tensor)

    pieces = []
    for g in range(groups):
        at = slice(g * HEAD_WIDTH, (g + 1) * HEAD_WIDTH)
        own = jnp.stack([keys[:, at], values[:, at]])
        pair = partner(own, "seq")
        two = shift(own, "seq", 2)
        swap = partner(two, "seq")
        far = lax.ppermute(pair, "seq", [(i, (i + 4) % count) for i in range(0, count, 2)])
        pieces.append((own, two, swap, pair, far))

    out = None
    last = []
    for g in range(groups):
        local = attend(shard[None], block_pos, queries, g, pieces[g])
        now = []
        for half in range(2):
            row = half * block_len
            now.append((local[half], row, me * groups + g))
            now.append((partner(local[half], "tensor"), row, (me ^ 1) * groups + g))
        if last:
            now = last + now
            last = []
        out = place(out, shape, now)
        for half in range(2):
            row = half * block_len
            for hop in range(1, tensor // 2):
                got = shift(local[half], "tensor", 2 * hop)
                owner = lax.rem(me - 2 * hop + tensor, tensor)
                last.append((got, row, owner * groups + g))
                last.append((partner(got, "tensor"), row, (owner ^ 1) * groups + g))
    return place(out, shape, last)


def solution(mesh):
    placed = (P("seq", "tensor"), P("seq", "tensor"), P("seq", "tensor"), P())
    return jax.shard_map(
        body, mesh=mesh, in_specs=placed, out_specs=P("seq", None), check_vma=False
    )
```

```python
import functools
import math

import jax
import jax.numpy as jnp
from jax import lax
from jax.experimental import pallas as pl
from jax.experimental.pallas import tpu as pltpu
from jax.sharding import PartitionSpec as P

QUERY_HEADS = 64
KEY_VALUE_HEADS = 8
HEAD_WIDTH = 128
GROUP = QUERY_HEADS // KEY_VALUE_HEADS
VISIBLE_SHARDS = 4


def shift(x, axis, distance):
    n = lax.axis_size(axis)
    return lax.ppermute(x, axis, [(i, (i + distance) % n) for i in range(n)])


def partner(x, axis):
    n = lax.axis_size(axis)
    return lax.ppermute(x, axis, [(i, i ^ 1) for i in range(n)])


def owner_column(me, tensor, hop, flip, groups, group, width):
    owner = lax.rem(me - 2 * hop + tensor, tensor)
    if flip:
        owner = owner + 1 - 2 * lax.rem(owner, 2)
    return pl.multiple_of((owner * groups + group) * width, width)


def attend_kernel(where_ref, pos_ref, q_ref, own_ref, two_ref, swap_ref, pair_ref, far_ref,
                  *rest, group, groups, qb, block_len, count, tensor, tile_heads):
    chunk_ref, out_ref, k_scr, v_scr, bias_scr, q_scr, q_sem, out_sem = rest[-8:]
    tok = 2 * block_len
    width = GROUP * HEAD_WIDTH
    rows = slice(qb * block_len, (qb + 1) * block_len)
    fetches = []
    for h in range(GROUP):
        col = group * width + h * HEAD_WIDTH
        fetches.append(pltpu.make_async_copy(
            q_ref.at[rows, col:col + HEAD_WIDTH],
            q_scr.at[h * block_len:(h + 1) * block_len], q_sem.at[h]))
    for fetch in fetches:
        fetch.start()
    shard = where_ref[0]
    odd = lax.rem(shard, 2)

    def fill(slot, ref):
        k_scr[:, slot * tok:(slot + 1) * tok] = ref[0].T
        v_scr[slot * tok:(slot + 1) * tok, :HEAD_WIDTH] = ref[1]

    fill(0, own_ref)
    fill(1, two_ref)
    fill(2, swap_ref)

    @pl.when(odd == 1)
    def _():
        fill(3, pair_ref)

    @pl.when(odd == 0)
    def _():
        fill(3, far_ref)

    v_scr[:, HEAD_WIDTH:] = jnp.ones((VISIBLE_SHARDS * tok, HEAD_WIDTH), jnp.bfloat16)
    backs = (0, 2, jnp.where(odd == 1, 3, 1), jnp.where(odd == 1, 1, 3))
    ahead = (lax.broadcasted_iota(jnp.int32, (block_len, block_len), 1)
             - lax.broadcasted_iota(jnp.int32, (block_len, block_len), 0))
    q_block = pos_ref[2 * shard + qb]
    for slot in range(VISIBLE_SHARDS):
        source = lax.rem(shard - backs[slot] + count, count)
        for kb in range(2):
            gap = (pos_ref[2 * source + kb] - q_block) * block_len
            at = (2 * slot + kb) * block_len
            bias_scr[:, at:at + block_len] = jnp.where(ahead + gap <= 0, 0.0, -1e30)

    scale = 1.0 / math.sqrt(HEAD_WIDTH)
    for fetch in fetches:
        fetch.wait()
    tile = tile_heads * block_len
    for t in range(GROUP // tile_heads):
        q = q_scr[t * tile:(t + 1) * tile, :]
        s = jnp.dot(q, k_scr[...], preferred_element_type=jnp.float32)
        s = s.reshape(tile_heads, block_len, -1) + bias_scr[...][None]
        s = s.reshape(tile, -1)
        top = jnp.max(s, axis=1, keepdims=True)
        w = jnp.exp((s - top) * scale).astype(jnp.bfloat16)
        o = jnp.dot(w, v_scr[...], preferred_element_type=jnp.float32)
        o = (o[:, :HEAD_WIDTH] / o[:, HEAD_WIDTH:]).astype(jnp.bfloat16)
        for i in range(tile_heads):
            h = t * tile_heads + i
            chunk_ref[:, h * HEAD_WIDTH:(h + 1) * HEAD_WIDTH] = (
                o[i * block_len:(i + 1) * block_len])
    col = owner_column(where_ref[1], tensor, 0, False, groups, group, width)
    store = pltpu.make_async_copy(chunk_ref, out_ref.at[rows, pl.ds(col, width)], out_sem)
    store.start()
    store.wait()


ANY = pl.BlockSpec(memory_space=pl.ANY)
SMEM = pl.BlockSpec(memory_space=pltpu.SMEM)
LOCAL = pl.BlockSpec(memory_space=pltpu.VMEM)
TILE_HEADS = 2


def resident(x):
    return pltpu.with_memory_space_constraint(x, pltpu.VMEM)


def attend(where, block_pos, queries, group, groups, qb, pieces, out, shape):
    tok = queries.shape[0]
    block_len = tok // 2
    width = GROUP * HEAD_WIDTH
    aliased = [] if out is None else [out]
    keys_seen = VISIBLE_SHARDS * tok
    return pl.pallas_call(
        functools.partial(
            attend_kernel, group=group, groups=groups, qb=qb, block_len=block_len,
            count=lax.axis_size("seq"), tensor=lax.axis_size("tensor"),
            tile_heads=TILE_HEADS),
        in_specs=[SMEM, SMEM, ANY] + [LOCAL] * 5 + [ANY] * len(aliased),
        out_specs=[LOCAL, ANY],
        out_shape=[pltpu.VMEM((block_len, width), jnp.bfloat16),
                   jax.ShapeDtypeStruct(shape, jnp.bfloat16)],
        input_output_aliases={8: 1} if aliased else {},
        scratch_shapes=[
            pltpu.VMEM((HEAD_WIDTH, keys_seen), jnp.bfloat16),
            pltpu.VMEM((keys_seen, 2 * HEAD_WIDTH), jnp.bfloat16),
            pltpu.VMEM((block_len, keys_seen), jnp.float32),
            pltpu.VMEM((GROUP * block_len, HEAD_WIDTH), jnp.bfloat16),
            pltpu.SemaphoreType.DMA((GROUP,)),
            pltpu.SemaphoreType.DMA,
        ],
        name=f"attend{group}{qb}",
    )(where, block_pos, queries, *[resident(p) for p in pieces], *aliased)


def place_kernel(where_ref, *refs, spots, groups, tensor):
    n = len(spots)
    out, sems = refs[-2:]
    copies = []
    for i, (chunk, (row, hop, flip, group)) in enumerate(zip(refs[:n], spots)):
        h, w = chunk.shape
        col = owner_column(where_ref[1], tensor, hop, flip, groups, group, w)
        copies.append(pltpu.make_async_copy(
            chunk, out.at[pl.ds(row, h), pl.ds(col, w)], sems.at[i]))
    for copy in copies:
        copy.start()
    for copy in copies:
        copy.wait()


def place(where, out, groups, entries):
    n = len(entries)
    return pl.pallas_call(
        functools.partial(place_kernel, spots=tuple(e[1:] for e in entries), groups=groups,
                          tensor=lax.axis_size("tensor")),
        in_specs=[SMEM] + [LOCAL] * n + [ANY],
        out_specs=ANY,
        out_shape=jax.ShapeDtypeStruct(out.shape, jnp.bfloat16),
        input_output_aliases={n + 1: 0},
        scratch_shapes=[pltpu.SemaphoreType.DMA((n,))],
        name="place",
    )(where, *[resident(e[0]) for e in entries], out)


def body(queries, keys, values, block_pos):
    tok = queries.shape[0]
    block_len = tok // 2
    groups = keys.shape[1] // HEAD_WIDTH
    count = lax.axis_size("seq")
    tensor = lax.axis_size("tensor")
    where = jnp.stack([lax.axis_index("seq"), lax.axis_index("tensor")]).astype(jnp.int32)
    shape = (tok, queries.shape[1] * tensor)

    pieces = []
    for g in range(groups):
        at = slice(g * HEAD_WIDTH, (g + 1) * HEAD_WIDTH)
        own = jnp.stack([keys[:, at], values[:, at]])
        if pieces:
            own, _ = lax.optimization_barrier((own, pieces[-1][2]))
        pair = partner(own, "seq")
        two = shift(own, "seq", 2)
        pair, two = lax.optimization_barrier((pair, two))
        swap = partner(two, "seq")
        far = lax.ppermute(pair, "seq", [(i, (i + 4) % count) for i in range(0, count, 2)])
        pieces.append((own, two, swap, pair, far))

    out = None
    arrivals = []
    beside = []
    for g in range(groups):
        for qb in range(2):
            local, out = attend(where, block_pos, queries, g, groups, qb, pieces[g], out, shape)
            row = qb * block_len
            beside.append((partner(local, "tensor"), row, 0, True, g))
            arrivals.append([(shift(local, "tensor", 2 * hop), row, hop, False, g)
                             for hop in range(1, tensor // 2)])
    out = place(where, out, groups, beside)
    for now in arrivals:
        first = now[0][0]
        first, out = lax.optimization_barrier((first, out))
        now[0] = (first,) + now[0][1:]
        crossed = [(partner(e[0], "tensor"),) + e[1:3] + (True,) + e[4:] for e in now]
        out = place(where, out, groups, now + crossed)
    return out


def solution(mesh):
    placed = (P("seq", "tensor"), P("seq", "tensor"), P("seq", "tensor"), P())
    return jax.shard_map(
        body, mesh=mesh, in_specs=placed, out_specs=P("seq", None), check_vma=False
    )
```

```python
import functools
import math

import jax
import jax.numpy as jnp
from jax import lax
from jax.experimental import pallas as pl
from jax.experimental.pallas import tpu as pltpu
from jax.sharding import PartitionSpec as P


QUERY_HEADS = 64
KEY_VALUE_HEADS = 8
HEAD_WIDTH = 128
GROUP = QUERY_HEADS // KEY_VALUE_HEADS
VISIBLE_SHARDS = 4
TILE_HEADS = 2

ANY = pl.BlockSpec(memory_space=pl.ANY)
SMEM = pl.BlockSpec(memory_space=pltpu.SMEM)
LOCAL = pl.BlockSpec(memory_space=pltpu.VMEM)


def shift(x, axis, distance):
    n = lax.axis_size(axis)
    return lax.ppermute(x, axis, [(i, (i + distance) % n) for i in range(n)])


def partner(x, axis):
    n = lax.axis_size(axis)
    return lax.ppermute(x, axis, [(i, i ^ 1) for i in range(n)])


def resident(x):
    return pltpu.with_memory_space_constraint(x, pltpu.VMEM)


def prepare_kernel(pos_ref, q_ref, stack_ref, mask_ref, sems, *, chunks, block_len, count):
    copies = []
    for c in range(chunks):
        g, qb = c // 2, c % 2
        for h in range(GROUP):
            col = (g * GROUP + h) * HEAD_WIDTH
            copies.append(pltpu.make_async_copy(
                q_ref.at[qb * block_len:(qb + 1) * block_len, col:col + HEAD_WIDTH],
                stack_ref.at[c, h * block_len:(h + 1) * block_len, :HEAD_WIDTH],
                sems.at[c * GROUP + h]))
    for copy in copies:
        copy.start()
    ahead = (lax.broadcasted_iota(jnp.int32, (block_len, block_len), 1)
             - lax.broadcasted_iota(jnp.int32, (block_len, block_len), 0))
    unit = jnp.where(ahead == 0, 1.0, 0.0).astype(jnp.bfloat16)
    for c in range(chunks):
        for h in range(GROUP):
            stack_ref[c, h * block_len:(h + 1) * block_len, HEAD_WIDTH:] = unit
    shard = lax.axis_index("seq").astype(jnp.int32)
    for qb in range(2):
        q_block = pos_ref[2 * shard + qb]
        for back in range(VISIBLE_SHARDS):
            source = lax.rem(shard - back + count, count)
            for kb in range(2):
                gap = (pos_ref[2 * source + kb] - q_block) * block_len
                at = (2 * back + kb) * block_len
                mask_ref[qb * block_len:(qb + 1) * block_len, at:at + block_len] = jnp.where(
                    ahead + gap <= 0, 0.0, -1e30).astype(jnp.bfloat16)
    for copy in copies:
        copy.wait()


def prepare(block_pos, queries, groups):
    tok = queries.shape[0]
    block_len = tok // 2
    chunks = 2 * groups
    return pl.pallas_call(
        functools.partial(prepare_kernel, chunks=chunks, block_len=block_len,
                          count=lax.axis_size("seq")),
        in_specs=[SMEM, ANY],
        out_specs=[LOCAL, LOCAL],
        out_shape=[
            pltpu.VMEM((chunks, GROUP * block_len, HEAD_WIDTH + block_len), jnp.bfloat16),
            pltpu.VMEM((tok, VISIBLE_SHARDS * tok), jnp.bfloat16),
        ],
        scratch_shapes=[pltpu.SemaphoreType.DMA((chunks * GROUP,))],
        name="prepare",
    )(block_pos, queries)


def attend_kernel(stack_ref, mask_ref, *rest, chunk, block_len):
    pieces = rest[:VISIBLE_SHARDS]
    out_ref, k_scr, v_scr = rest[VISIBLE_SHARDS:]
    tok = 2 * block_len
    qb = chunk % 2
    for slot, ref in enumerate(pieces):
        k_scr[:HEAD_WIDTH, slot * tok:(slot + 1) * tok] = ref[0].T
        v_scr[slot * tok:(slot + 1) * tok, :HEAD_WIDTH] = ref[1]
    v_scr[:, HEAD_WIDTH:] = jnp.ones((VISIBLE_SHARDS * tok, HEAD_WIDTH), jnp.bfloat16)
    k_scr[HEAD_WIDTH:, :] = mask_ref[qb * block_len:(qb + 1) * block_len, :]
    scale = math.log2(math.e) / math.sqrt(HEAD_WIDTH)
    tile = TILE_HEADS * block_len
    steps = GROUP // TILE_HEADS

    def scores(t):
        q = stack_ref[chunk, t * tile:(t + 1) * tile, :]
        return jnp.dot(q, k_scr[...], preferred_element_type=jnp.float32)

    def finish(t, s):
        top = jnp.max(s, axis=1, keepdims=True)
        w = jnp.exp2((s - top) * scale).astype(jnp.bfloat16)
        o = jnp.dot(w, v_scr[...], preferred_element_type=jnp.float32)
        o = (o[:, :HEAD_WIDTH] / o[:, HEAD_WIDTH:]).astype(jnp.bfloat16)
        for i in range(TILE_HEADS):
            h = t * TILE_HEADS + i
            out_ref[:, h * HEAD_WIDTH:(h + 1) * HEAD_WIDTH] = (
                o[i * block_len:(i + 1) * block_len])

    s = scores(0)
    for t in range(steps):
        following = scores(t + 1) if t + 1 < steps else None
        finish(t, s)
        s = following


def attend(stack, mask, chunk, pieces):
    block_len = mask.shape[0] // 2
    seen = mask.shape[1]
    return pl.pallas_call(
        functools.partial(attend_kernel, chunk=chunk, block_len=block_len),
        in_specs=[LOCAL] * (2 + VISIBLE_SHARDS),
        out_specs=LOCAL,
        out_shape=pltpu.VMEM((block_len, GROUP * HEAD_WIDTH), jnp.bfloat16),
        scratch_shapes=[
            pltpu.VMEM((HEAD_WIDTH + block_len, seen), jnp.bfloat16),
            pltpu.VMEM((seen, 2 * HEAD_WIDTH), jnp.bfloat16),
        ],
    )(resident(stack), resident(mask), *[resident(p) for p in pieces])


def place_kernel(*refs, spots, groups, tensor):
    n = len(spots)
    out, sems = refs[-2:]
    me = lax.axis_index("tensor").astype(jnp.int32)
    copies = []
    for i, (ref, (row, hop, flip, group)) in enumerate(zip(refs[:n], spots)):
        h, w = ref.shape
        owner = lax.rem(me - 2 * hop + tensor, tensor)
        if flip:
            owner = owner + 1 - 2 * lax.rem(owner, 2)
        col = pl.multiple_of((owner * groups + group) * w, w)
        copies.append(pltpu.make_async_copy(
            ref, out.at[pl.ds(row, h), pl.ds(col, w)], sems.at[i]))
    for copy in copies:
        copy.start()
    for copy in copies:
        copy.wait()


def place(out, shape, groups, entries):
    n = len(entries)
    aliased = [] if out is None else [out]
    return pl.pallas_call(
        functools.partial(place_kernel, spots=tuple(e[1:] for e in entries), groups=groups,
                          tensor=lax.axis_size("tensor")),
        in_specs=[LOCAL] * n + [ANY] * len(aliased),
        out_specs=ANY,
        out_shape=jax.ShapeDtypeStruct(shape, jnp.bfloat16),
        input_output_aliases={n: 0} if aliased else {},
        scratch_shapes=[pltpu.SemaphoreType.DMA((n,))],
        name="place",
    )(*[resident(e[0]) for e in entries], *aliased)


def body(queries, keys, values, block_pos):
    tok = queries.shape[0]
    block_len = tok // 2
    groups = keys.shape[1] // HEAD_WIDTH
    tensor = lax.axis_size("tensor")
    shape = (tok, queries.shape[1] * tensor)

    pieces = []
    for g in range(groups):
        at = slice(g * HEAD_WIDTH, (g + 1) * HEAD_WIDTH)
        own = jnp.stack([keys[:, at], values[:, at]])
        behind = [own]
        for back in range(1, VISIBLE_SHARDS):
            behind.append(shift(own, "seq", back))
        pieces.append(behind)
    stack, mask = prepare(block_pos, queries, groups)

    arrivals = []
    beside = []
    for chunk in range(2 * groups):
        g, qb = chunk // 2, chunk % 2
        row = qb * block_len
        local = attend(stack, mask, chunk, pieces[g])
        now = []
        for hop in range(1, tensor // 2):
            now.append((shift(local, "tensor", 2 * hop), row, hop, False, g))
        arrivals.append(now)
        beside.append((local, row, 0, False, g))
        beside.append((partner(local, "tensor"), row, 0, True, g))
    out = place(None, shape, groups, beside)
    for now in arrivals:
        if now:
            first, out = lax.optimization_barrier((now[0][0], out))
            now[0] = (first,) + now[0][1:]
            crossed = [(partner(e[0], "tensor"),) + e[1:3] + (True,) + e[4:] for e in now]
            out = place(out, shape, groups, now + crossed)
    return out


def solution(mesh):
    placed = (P("seq", "tensor"), P("seq", "tensor"), P("seq", "tensor"), P())

    return jax.shard_map(
        body, mesh=mesh, in_specs=placed, out_specs=P("seq", None), check_vma=False
    )
```

```python
import functools
import math

import jax
import jax.numpy as jnp
from jax import lax
from jax.experimental import pallas as pl
from jax.experimental.pallas import tpu as pltpu
from jax.sharding import PartitionSpec as P


QUERY_HEADS = 64
KEY_VALUE_HEADS = 8
HEAD_WIDTH = 128
GROUP = QUERY_HEADS // KEY_VALUE_HEADS
VISIBLE_SHARDS = 4
TILE_HEADS = 2

ANY = pl.BlockSpec(memory_space=pl.ANY)
SMEM = pl.BlockSpec(memory_space=pltpu.SMEM)
LOCAL = pl.BlockSpec(memory_space=pltpu.VMEM)


def shift(x, axis, distance):
    n = lax.axis_size(axis)
    return lax.ppermute(x, axis, [(i, (i + distance) % n) for i in range(n)])


def partner(x, axis):
    n = lax.axis_size(axis)
    return lax.ppermute(x, axis, [(i, i ^ 1) for i in range(n)])


def resident(x):
    return pltpu.with_memory_space_constraint(x, pltpu.VMEM)


def build_mask(pos_ref, mask_ref, block_len, count):
    ahead = (lax.broadcasted_iota(jnp.int32, (block_len, block_len), 1)
             - lax.broadcasted_iota(jnp.int32, (block_len, block_len), 0))
    shard = lax.axis_index("seq").astype(jnp.int32)
    odd = lax.rem(shard, 2)
    backs = (0, 2, 1 + 2 * odd, 3 - 2 * odd)
    for qb in range(2):
        q_block = pos_ref[2 * shard + qb]
        for slot, back in enumerate(backs):
            source = lax.rem(shard - back + count, count)
            for kb in range(2):
                gap = (pos_ref[2 * source + kb] - q_block) * block_len
                at = (2 * slot + kb) * block_len
                mask_ref[qb * block_len:(qb + 1) * block_len, at:at + block_len] = jnp.where(
                    ahead + gap <= 0, 0.0, -1e30).astype(jnp.bfloat16)


def prepare_kernel(pos_ref, q_ref, *rest, group, block_len, count):
    stacks = rest[:2]
    sems = rest[-1]
    copies = []
    for qb in range(2):
        for h in range(GROUP):
            col = (group * GROUP + h) * HEAD_WIDTH
            copies.append(pltpu.make_async_copy(
                q_ref.at[qb * block_len:(qb + 1) * block_len, col:col + HEAD_WIDTH],
                stacks[qb].at[h * block_len:(h + 1) * block_len],
                sems.at[qb * GROUP + h]))
    for copy in copies:
        copy.start()
    if group == 0:
        build_mask(pos_ref, rest[2], block_len, count)
    for copy in copies:
        copy.wait()


def prepare(block_pos, queries, group):
    tok = queries.shape[0]
    block_len = tok // 2
    masks = 1 if group == 0 else 0
    return pl.pallas_call(
        functools.partial(prepare_kernel, group=group, block_len=block_len,
                          count=lax.axis_size("seq")),
        in_specs=[SMEM, ANY],
        out_specs=[LOCAL] * (2 + masks),
        out_shape=[pltpu.VMEM((GROUP * block_len, HEAD_WIDTH), jnp.bfloat16)] * 2
        + [pltpu.VMEM((tok, VISIBLE_SHARDS * tok), jnp.bfloat16)] * masks,
        scratch_shapes=[pltpu.SemaphoreType.DMA((2 * GROUP,))],
    )(block_pos, queries)


def attend_kernel(stack_ref, mask_ref, *rest, chunk, block_len):
    own_ref, two_ref, swap_ref, pair_ref, far_ref, out_ref, k_scr, v_scr, q_scr = rest
    tok = 2 * block_len
    qb = chunk % 2

    def fill(slot, ref):
        k_scr[:HEAD_WIDTH, slot * tok:(slot + 1) * tok] = ref[0].T
        v_scr[slot * tok:(slot + 1) * tok, :HEAD_WIDTH] = ref[1]

    fill(0, own_ref)
    fill(1, two_ref)
    fill(2, swap_ref)
    odd = lax.rem(lax.axis_index("seq").astype(jnp.int32), 2)

    @pl.when(odd == 1)
    def _():
        fill(3, pair_ref)

    @pl.when(odd == 0)
    def _():
        fill(3, far_ref)

    v_scr[:, HEAD_WIDTH:] = jnp.ones((VISIBLE_SHARDS * tok, HEAD_WIDTH), jnp.bfloat16)
    k_scr[HEAD_WIDTH:, :] = mask_ref[qb * block_len:(qb + 1) * block_len, :]
    unit = jnp.where(lax.broadcasted_iota(jnp.int32, (block_len, block_len), 1)
                     == lax.broadcasted_iota(jnp.int32, (block_len, block_len), 0),
                     1.0, 0.0).astype(jnp.bfloat16)
    q_scr[:, :HEAD_WIDTH] = stack_ref[...]
    for h in range(GROUP):
        q_scr[h * block_len:(h + 1) * block_len, HEAD_WIDTH:] = unit
    scale = math.log2(math.e) / math.sqrt(HEAD_WIDTH)
    tile = TILE_HEADS * block_len
    steps = GROUP // TILE_HEADS

    def scores(t):
        q = q_scr[t * tile:(t + 1) * tile, :]
        return jnp.dot(q, k_scr[...], preferred_element_type=jnp.float32)

    def finish(t, s):
        top = jnp.max(s, axis=1, keepdims=True)
        w = jnp.exp2((s - top) * scale).astype(jnp.bfloat16)
        o = jnp.dot(w, v_scr[...], preferred_element_type=jnp.float32)
        o = (o[:, :HEAD_WIDTH] / o[:, HEAD_WIDTH:]).astype(jnp.bfloat16)
        for i in range(TILE_HEADS):
            h = t * TILE_HEADS + i
            out_ref[:, h * HEAD_WIDTH:(h + 1) * HEAD_WIDTH] = (
                o[i * block_len:(i + 1) * block_len])

    s = scores(0)
    for t in range(steps):
        following = scores(t + 1) if t + 1 < steps else None
        finish(t, s)
        s = following


def attend(stack, mask, chunk, pieces):
    block_len = mask.shape[0] // 2
    seen = mask.shape[1]
    return pl.pallas_call(
        functools.partial(attend_kernel, chunk=chunk, block_len=block_len),
        in_specs=[LOCAL] * (2 + len(pieces)),
        out_specs=LOCAL,
        out_shape=pltpu.VMEM((block_len, GROUP * HEAD_WIDTH), jnp.bfloat16),
        scratch_shapes=[
            pltpu.VMEM((HEAD_WIDTH + block_len, seen), jnp.bfloat16),
            pltpu.VMEM((seen, 2 * HEAD_WIDTH), jnp.bfloat16),
            pltpu.VMEM((GROUP * block_len, HEAD_WIDTH + block_len), jnp.bfloat16),
        ],
    )(resident(stack), resident(mask), *[resident(p) for p in pieces])


def place_kernel(*refs, spots, groups, tensor):
    n = len(spots)
    out, sems = refs[-2:]
    me = lax.axis_index("tensor").astype(jnp.int32)
    copies = []
    for i, (ref, (row, hop, flip, group)) in enumerate(zip(refs[:n], spots)):
        h, w = ref.shape
        owner = lax.rem(me - 2 * hop + tensor, tensor)
        if flip:
            owner = owner + 1 - 2 * lax.rem(owner, 2)
        col = pl.multiple_of((owner * groups + group) * w, w)
        copies.append(pltpu.make_async_copy(
            ref, out.at[pl.ds(row, h), pl.ds(col, w)], sems.at[i]))
    for copy in copies:
        copy.start()
    for copy in copies:
        copy.wait()


def place(out, shape, groups, entries):
    n = len(entries)
    aliased = [] if out is None else [out]
    return pl.pallas_call(
        functools.partial(place_kernel, spots=tuple(e[1:] for e in entries), groups=groups,
                          tensor=lax.axis_size("tensor")),
        in_specs=[LOCAL] * n + [ANY] * len(aliased),
        out_specs=ANY,
        out_shape=jax.ShapeDtypeStruct(shape, jnp.bfloat16),
        input_output_aliases={n: 0} if aliased else {},
        scratch_shapes=[pltpu.SemaphoreType.DMA((n,))],
        name="place",
    )(*[resident(e[0]) for e in entries], *aliased)


def body(queries, keys, values, block_pos):
    tok = queries.shape[0]
    block_len = tok // 2
    groups = keys.shape[1] // HEAD_WIDTH
    tensor = lax.axis_size("tensor")
    count = lax.axis_size("seq")
    shape = (tok, queries.shape[1] * tensor)

    pieces = []
    for g in range(groups):
        at = slice(g * HEAD_WIDTH, (g + 1) * HEAD_WIDTH)
        own = jnp.stack([keys[:, at], values[:, at]])
        pair = partner(own, "seq")
        two = shift(own, "seq", 2)
        swap = partner(two, "seq")
        far = lax.ppermute(pair, "seq", [(i, (i + 4) % count) for i in range(0, count, 2)])
        pieces.append((own, two, swap, pair, far))
    *stacks, mask = prepare(block_pos, queries, 0)
    for g in range(1, groups):
        stacks += prepare(block_pos, queries, g)

    arrivals = []
    beside = []
    for chunk in range(2 * groups):
        g, qb = chunk // 2, chunk % 2
        row = qb * block_len
        local = attend(stacks[chunk], mask, chunk, pieces[g])
        now = []
        for hop in range(1, tensor // 2):
            now.append((shift(local, "tensor", 2 * hop), row, hop, False, g))
        arrivals.append(now)
        beside.append((local, row, 0, False, g))
        beside.append((partner(local, "tensor"), row, 0, True, g))

    def crossed(chunk):
        return [(partner(e[0], "tensor"),) + e[1:3] + (True,) + e[4:]
                for e in arrivals[chunk]]

    early = 2 * groups - 2
    out = None
    if early:
        out = place(None, shape, groups, beside[:2 * early])
    batch = beside[2 * early:]
    if early:
        batch = batch + arrivals[0] + crossed(0)
    out = place(out, shape, groups, batch)
    held = []
    for chunk in range(1 if early else 0, 2 * groups):
        now = arrivals[chunk]
        if now:
            first, out = lax.optimization_barrier((now[0][0], out))
            now[0] = (first,) + now[0][1:]
            held = held + now + crossed(chunk)
            if chunk >= early:
                out = place(out, shape, groups, held)
                held = []
    return out


def solution(mesh):
    placed = (P("seq", "tensor"), P("seq", "tensor"), P("seq", "tensor"), P())

    return jax.shard_map(
        body, mesh=mesh, in_specs=placed, out_specs=P("seq", None), check_vma=False
    )
```
